32 devices in a mesh: member: 2 (over x), graph: 8 (over z, y), chan: 2 (over core).
Axes of the slice: x: 2, y: 2, z: 4, core: 2. Of those that a mesh axis runs over, the one named last changes fastest.
Arguments:
- grid_state: bfloat16 [16384, 256], P(('member', 'graph')), parts along dimension 0, may hold values from -6 to 6
- w_src: bfloat16 [256, 512], P(None, 'chan'), may hold values from -0.375 to 0.375
- bias_src: float32 [512], P('chan'), may hold values from -3 to 3
- mesh_embed: bfloat16 [5120, 512], P('graph', 'chan'), may hold values from -6 to 6
- w_node: bfloat16 [512, 512], P('chan'), may hold values from -0.25 to 0.25
- w_dec: bfloat16 [512, 256], P('chan'), may hold values from -0.125 to 0.125
- slot_src: int32 [8, 8, 1024], P('graph'), may hold values from 0 to 1023, as said below
- slot_dst: int32 [8, 8, 1024], P(None, 'graph'), may hold values from 0 to 639, as said below
- slot_count: int32 [8, 8], replicated, may hold values from 1 to 1024, as said below
Outputs:
- grid_out: bfloat16 [16384, 256], P(('member', 'graph'), 'chan'), parts along dimension 0
The draws below stay inside these ranges and needn't reach their ends.
There are 2 independent parts, one for each index of `member`. The reference program is written for one: setup_inputs(seed, part) draws one part's arguments, and reference() takes and returns one part's arrays. A program takes and returns all parts, laid end to end along the dimension named above; an argument that names none is the same for every part. Nothing has to cross between parts.
Inputs may be any that keep to these rules, and one draw needn't show every extreme that they name: `slot_src`: slots at or past the live count hold arbitrary values in the same range. `slot_dst`: slots at or past the live count hold arbitrary values in the same range. slot_count[s, d] counts the live leading slots of the 1024 from shard s to shard d; in every draw some receiving shard has all 1024 slots live from every sender.
All inputs are finite; a program needn't handle non-finite values.
Results may differ from the reference program's by a relative error of at most 0.0056.
Values may be sent and summed in bfloat16 or wider, within the bound.
A program may use at most 64 MiB of HBM per device.

```python
import jax
import jax.numpy as jnp
from jax import lax

C = 256
H = 512
GD = 1024
MD = 640
CAP = 1024
G = 8192
M = 5120
N_GRAPH = 8


def edge_tables(key):
    owners = jnp.arange(N_GRAPH, dtype=jnp.int32)
    offset = jnp.abs(owners[:, None] - owners[None, :])
    cycle_gap = jnp.minimum(offset, N_GRAPH - offset)
    near_bits = jax.random.randint(jax.random.fold_in(key, 12), (N_GRAPH, N_GRAPH), 0, 1 << 20)
    near_count = CAP // 2 + near_bits % (CAP - CAP // 2 + 1)
    levels = jax.random.randint(jax.random.fold_in(key, 11), (N_GRAPH,), 1, 5)
    tail_top = jnp.maximum(levels * (CAP // 16), 1)
    tail_bits = jax.random.randint(jax.random.fold_in(key, 14), (N_GRAPH, N_GRAPH), 0, 1 << 20)
    tail_pick = jax.random.randint(jax.random.fold_in(key, 15), (N_GRAPH, N_GRAPH), 0, 8)
    tail_count = jnp.where(tail_pick == 0, 1 + tail_bits % tail_top[None, :], 1)
    counts = jnp.where(cycle_gap <= 2, near_count, tail_count)
    fullest = jax.random.randint(jax.random.fold_in(key, 13), (), 0, N_GRAPH)
    return jnp.where(owners[None, :] == fullest, CAP, counts).astype(jnp.int32)


def draw_slot_count(key, part):
    return edge_tables(key)


def draw_slot_src(key, part):
    return jax.random.randint(jax.random.fold_in(key, 21), (N_GRAPH, N_GRAPH, CAP), 0, GD).astype(jnp.int32)


def draw_slot_dst(key, part):
    return jax.random.randint(jax.random.fold_in(key, 31), (N_GRAPH, N_GRAPH, CAP), 0, MD).astype(jnp.int32)


def block_scale(own_key, shape, shards, low, high):
    gain = 1.0
    for axis_at, blocks in shards:
        steps = jax.random.uniform(jax.random.fold_in(jax.random.fold_in(own_key, 6), axis_at), (blocks,), jnp.float32, low / len(shards), high / len(shards))
        gain = gain * jnp.repeat(jnp.exp(steps), shape[axis_at] // blocks).reshape((-1,) + (1,) * (len(shape) - 1 - axis_at))
    return gain


def scatter_about(rng, extent, spread, reach, cuts=(), kind=jnp.bfloat16):
    gain = block_scale(rng, extent, cuts, -0.22, 0.18) if cuts else 1.0
    array = jax.random.normal(rng, extent, jnp.float32) * spread * gain
    return jnp.minimum(jnp.maximum(array, -reach), reach).astype(kind)


def setup_inputs(seed: int = 0, part: int = 0) -> dict:
    arg_keys = jax.random.split(jax.random.key(seed), 10)
    own_keys = jax.random.split(jax.random.fold_in(arg_keys[9], part), 10)
    grid_state = scatter_about(own_keys[0], (G, C), 1.0, 6.0, ((0, 8),))
    w_src = scatter_about(arg_keys[1], (C, H), C ** -0.5, 0.375, ((1, 2),))
    bias_src = scatter_about(arg_keys[2], (H,), 0.5, 3.0, ((0, 2),), jnp.float32)
    mesh_embed = scatter_about(arg_keys[3], (M, H), 1.0, 6.0, ((0, 8), (1, 2)))
    w_node = scatter_about(arg_keys[4], (H, H), H ** -0.5, 0.25, ((0, 2),))
    w_dec = scatter_about(arg_keys[5], (H, C), (4 * H) ** -0.5, 0.125, ((0, 2),))
    slot_src = draw_slot_src(jax.random.fold_in(arg_keys[9], 71), part)
    slot_dst = draw_slot_dst(jax.random.fold_in(arg_keys[9], 71), part)
    slot_count = draw_slot_count(jax.random.fold_in(arg_keys[9], 71), part)
    return {"grid_state": grid_state, "w_src": w_src, "bias_src": bias_src, "mesh_embed": mesh_embed, "w_node": w_node, "w_dec": w_dec, "slot_src": slot_src, "slot_dst": slot_dst, "slot_count": slot_count}


def reference(grid_state, w_src, bias_src, mesh_embed, w_node, w_dec, slot_src, slot_dst, slot_count):
    positions = jnp.arange(CAP, dtype=jnp.int32)
    owners = jnp.arange(N_GRAPH, dtype=jnp.int32)

    def send_part(aggregate, sender):
        picked = jnp.take(grid_state, (sender * GD + slot_src[sender]).reshape(-1), axis=0)
        messages = jax.nn.silu(jnp.dot(picked, w_src, preferred_element_type=jnp.float32) + bias_src).astype(jnp.bfloat16)
        usable = (positions[None, :] < slot_count[sender][:, None]).reshape(-1)
        mesh_ids = (owners[:, None] * MD + slot_dst[sender]).reshape(-1).astype(jnp.int32)
        terms = jnp.where(usable[:, None], messages.astype(jnp.float32), jnp.zeros((), jnp.float32))
        return aggregate + jax.ops.segment_sum(terms, mesh_ids, num_segments=N_GRAPH * MD), None

    aggregate, unused = lax.scan(send_part, jnp.zeros((N_GRAPH * MD, H), jnp.float32), owners)
    hidden_pre = jnp.dot(aggregate.astype(jnp.bfloat16), w_node, preferred_element_type=jnp.float32)
    latent = (mesh_embed.astype(jnp.float32) + jax.nn.silu(hidden_pre)).astype(jnp.bfloat16)
    projected = jnp.dot(latent, w_dec, preferred_element_type=jnp.float32).astype(jnp.bfloat16)

    def decode_part(sender):
        usable = (positions[None, :] < slot_count[sender][:, None]).reshape(-1)
        mesh_ids = (owners[:, None] * MD + slot_dst[sender]).reshape(-1).astype(jnp.int32)
        returned = jnp.where(usable[:, None], jnp.take(projected, mesh_ids, axis=0).astype(jnp.float32), jnp.zeros((), jnp.float32))
        decoded = jax.ops.segment_sum(returned, slot_src[sender].reshape(-1).astype(jnp.int32), num_segments=GD)
        own_rows = lax.dynamic_slice_in_dim(grid_state, (sender * GD).astype(jnp.int32), GD, 0)
        return (own_rows.astype(jnp.float32) + decoded).astype(jnp.bfloat16)

    return lax.map(decode_part, owners).reshape(N_GRAPH * GD, C)
```

```python
import functools
import math

import jax
import jax.numpy as jnp
from jax import lax
from jax.experimental import pallas as pl
from jax.experimental.pallas import tpu as pltpu
from jax.sharding import PartitionSpec as P

VMEM_BUDGET = 48 * 2**20
MESH = pl.DeviceIdType.MESH
NT = (((1,), (1,)), ((), ()))


def edge_network(source_rows, w_src, bias_src):
    return jax.nn.silu(
        jnp.dot(source_rows, w_src, preferred_element_type=jnp.float32) + bias_src
    ).astype(jnp.bfloat16)


def segment_rows(values, indices, usable, row_count):
    slot_total = values.shape[0]
    width = values.shape[1]
    block_len = math.gcd(slot_total, 2048)
    block_count = slot_total // block_len
    targets = jnp.where(usable, indices, -1).reshape(block_count, block_len)
    pieces = values.reshape(block_count, block_len, width)
    row_ids = jnp.arange(row_count, dtype=jnp.int32)

    def add_block(summed, scan_item):
        row_target, piece_vals = scan_item
        one_hot = (row_ids[:, None] == row_target[None, :]).astype(jnp.bfloat16)
        return (summed + jnp.dot(one_hot, piece_vals, preferred_element_type=jnp.float32), None)

    result, unused = lax.scan(
        add_block, jnp.zeros((row_count, width), jnp.float32), (targets, pieces)
    )
    return result


def on_device(
    grid_state, w_src, bias_src, mesh_embed, w_node, w_dec, slot_src, slot_dst, slot_count
):
    peers = lax.axis_size("graph")
    own_index = lax.axis_index("graph")
    core_index = lax.axis_index("chan")
    capacity = slot_src.shape[2]
    positions = jnp.arange(capacity, dtype=jnp.int32)
    grid_rows = grid_state.shape[0]
    mesh_rows = mesh_embed.shape[0]
    sent_counts = lax.dynamic_slice_in_dim(slot_count, own_index, 1, 0)[0]
    recv_counts = lax.dynamic_slice_in_dim(slot_count, own_index, 1, 1)[:, 0]
    half_slots = capacity // 2
    chosen = lax.dynamic_slice_in_dim(slot_src[0], core_index * half_slots, half_slots, 1)
    picked = jnp.take(grid_state, chosen.reshape(-1), axis=0).reshape(
        peers, half_slots, grid_state.shape[1]
    )
    arrived = lax.all_to_all(picked, "graph", split_axis=0, concat_axis=0, tiled=True)
    joined = lax.all_gather(arrived, "chan", axis=1, tiled=True)
    messages = edge_network(joined.reshape(peers * capacity, grid_state.shape[1]), w_src, bias_src)
    arrive_ok = (positions[None, :] < recv_counts[:, None]).reshape(-1)
    dst_rows = slot_dst[:, 0, :].reshape(-1)
    aggregate = segment_rows(messages, dst_rows, arrive_ok, mesh_rows)
    partial_hidden = jnp.dot(
        aggregate.astype(jnp.bfloat16), w_node, preferred_element_type=jnp.float32
    )
    hidden_pre = lax.psum_scatter(partial_hidden, "chan", scatter_dimension=1, tiled=True)
    latent = (mesh_embed.astype(jnp.float32) + jax.nn.silu(hidden_pre)).astype(jnp.bfloat16)
    partial_proj = jnp.dot(latent, w_dec, preferred_element_type=jnp.float32)
    projected = lax.psum_scatter(partial_proj, "chan", scatter_dimension=1, tiled=True).astype(
        jnp.bfloat16
    )
    returned = jnp.take(projected, dst_rows, axis=0).reshape(peers, capacity, projected.shape[1])
    came_back = lax.all_to_all(returned, "graph", split_axis=0, concat_axis=0, tiled=True).reshape(
        peers * capacity, projected.shape[1]
    )
    send_ok = (positions[None, :] < sent_counts[:, None]).reshape(-1)
    decoded = segment_rows(came_back, slot_src[0].reshape(-1), send_ok, grid_rows)
    width_half = decoded.shape[1]
    own_cols = lax.dynamic_slice_in_dim(grid_state, core_index * width_half, width_half, 1)
    return (own_cols.astype(jnp.float32) + decoded).astype(jnp.bfloat16)


def silu(v):
    half = 0.5 * v
    return half + half * jnp.tanh(half)


def one_hot(first, rows, indices):
    row_ids = lax.broadcasted_iota(jnp.int32, (rows, indices.shape[1]), 0) + first
    return jnp.where(row_ids == indices, 1.0, 0.0).astype(jnp.bfloat16)


def graph_kernel(
    peers,
    x_ref, w_src_ref, bias_ref, embed_ref, w_node_ref, w_dec_ref, src_ref, dst_ref,
    out_ref,
    x_all, src_in, dst_in, w_src_all, bias_all, embed_all, w_node_all, w_dec_all,
    enc, dec, hot, agg, proj, proj_all, total,
    local_sem, par_send, par_recv, idx_send, idx_recv,
    xz_send, xy_send, xi_recv, xm_send, xm_recv,
    pz_send, pz_recv, py_send, py_recv, pm_send, pm_recv, pr_send, pr_recv,
):
    lines = peers // 2
    me = lax.axis_index("graph")
    core = lax.axis_index("chan")
    mate = 1 - core
    line, side = me // 2, me % 2
    other = line * 2 + (1 - side)
    grid_rows, chans = x_ref.shape
    half_grid = grid_rows // 2
    mesh_rows = embed_ref.shape[0]
    half_mesh = mesh_rows // 2
    cols = chans // 2
    tile = enc.shape[3]
    tiles = grid_rows // tile

    def remote(src, dst, send, recv, graph, chan):
        return pltpu.make_async_remote_copy(
            src_ref=src, dst_ref=dst, send_sem=send, recv_sem=recv,
            device_id={"graph": graph, "chan": chan}, device_id_type=MESH,
        )

    barrier = pltpu.get_barrier_semaphore()
    for step in range(peers):
        for chan in range(2):
            if step == 0 and chan == 0:
                continue
            pl.semaphore_signal(
                barrier, inc=1,
                device_id={"graph": (me + step) % peers, "chan": (core + chan) % 2},
                device_id_type=MESH,
            )
    locals_ = [
        pltpu.make_async_copy(x_ref, x_all.at[me], local_sem.at[0]),
        pltpu.make_async_copy(w_src_ref, w_src_all.at[core], local_sem.at[1]),
        pltpu.make_async_copy(bias_ref, bias_all.at[core], local_sem.at[2]),
        pltpu.make_async_copy(
            embed_ref.at[pl.ds(pl.multiple_of(core * half_mesh, half_mesh), half_mesh)],
            embed_all.at[core], local_sem.at[3]),
        pltpu.make_async_copy(w_node_ref, w_node_all.at[core], local_sem.at[4]),
        pltpu.make_async_copy(w_dec_ref, w_dec_all.at[core], local_sem.at[5]),
        pltpu.make_async_copy(src_ref.at[me], src_in.at[me], local_sem.at[6]),
        pltpu.make_async_copy(dst_ref.at[me], dst_in.at[me], local_sem.at[7]),
    ]
    for copy in locals_:
        copy.start()
    pl.semaphore_wait(barrier, 2 * peers - 1)

    idx_copies = []
    for step in range(1, peers):
        to = (me + step) % peers
        for at, (ref, into) in enumerate(((src_ref, src_in), (dst_ref, dst_in))):
            copy = remote(
                ref.at[to], into.at[me], idx_send.at[at, step], idx_recv.at[at, step], to, core
            )
            copy.start()
            idx_copies.append(copy)

    def x_block(shard, half):
        return x_all.at[shard, pl.ds(pl.multiple_of(half * half_grid, half_grid), half_grid)]

    def x_copy(shard, send, recv_at, graph):
        ref = x_block(shard, core)
        return remote(ref, ref, send, xi_recv.at[recv_at], graph, core)

    own_half = x_ref.at[pl.ds(pl.multiple_of(core * half_grid, half_grid), half_grid)]
    y_copies = [remote(own_half, x_block(me, core), xy_send.at[0], xi_recv.at[0], other, core)]
    y_copies[0].start()
    z_copies = {}
    z_order = [k for pair in zip(range(1, lines), range(lines - 1, 0, -1)) for k in pair]
    z_order = list(dict.fromkeys(z_order))
    for k in z_order:
        to = ((line + k) % lines) * 2 + side
        z_copies[k] = remote(
            own_half, x_block(me, core), xz_send.at[k], xi_recv.at[k], to, core
        )
        z_copies[k].start()

    mate_rows = pl.ds(pl.multiple_of(mate * half_mesh, half_mesh), half_mesh)
    par_copies = [
        remote(w_src_ref, w_src_all.at[core], par_send.at[0], par_recv.at[0], me, mate),
        remote(bias_ref, bias_all.at[core], par_send.at[1], par_recv.at[1], me, mate),
        remote(embed_ref.at[mate_rows], embed_all.at[core], par_send.at[2], par_recv.at[2], me, mate),
        remote(w_node_ref, w_node_all.at[core], par_send.at[3], par_recv.at[3], me, mate),
        remote(w_dec_ref, w_dec_all.at[core], par_send.at[4], par_recv.at[4], me, mate),
    ]
    for copy in par_copies:
        copy.start()
    for copy in locals_:
        copy.wait()
    for copy in idx_copies:
        copy.wait()

    def build_enc(shard, carry):
        hot[: half_mesh, :] = one_hot(core * half_mesh, half_mesh, dst_ref[shard])
        for t in range(tiles):
            picks = one_hot(t * tile, tile, src_in[shard])
            enc[shard, t] = lax.dot_general(
                hot[: half_mesh, :], picks, NT, preferred_element_type=jnp.float32
            ).astype(jnp.bfloat16)
        return carry

    def build_dec(shard, carry):
        hot[...] = one_hot(0, mesh_rows, dst_in[shard])
        for t in range(grid_rows // 256):
            picks = one_hot(t * 256, 256, src_ref[shard])
            dec[shard, t * 256 : (t + 1) * 256, :] = lax.dot_general(
                picks, hot[...], NT, preferred_element_type=jnp.float32
            ).astype(jnp.bfloat16)
        return carry

    def shard_of(event):
        if event == 0:
            return other
        k = event if event < lines else event - lines + 1
        from_line = (line + lines - k) % lines
        return from_line * 2 + (side if event < lines else 1 - side)

    mate_copies = {}

    def relay(event):
        shard = shard_of(event)
        x_copy(shard, xy_send.at[0], event, other).wait_recv()
        if 0 < event < lines:
            copy = x_copy(shard, xy_send.at[event], lines - 1 + event, other)
            copy.start()
            y_copies.append(copy)
        ref = x_block(shard, core)
        copy = remote(ref, ref, xm_send.at[event], xm_recv.at[event], me, mate)
        copy.start()
        mate_copies[event] = copy

    def encode(shard, t):
        for h in range(2):
            pre = jnp.dot(
                x_all[shard, t * tile : (t + 1) * tile, :], w_src_all[h],
                preferred_element_type=jnp.float32,
            ) + bias_all[h]
            part = jnp.dot(
                enc[shard, t], silu(pre).astype(jnp.bfloat16), preferred_element_type=jnp.float32
            )
            agg[h] += part

    def encode_event(event):
        mate_copies[event].wait_recv()
        for t in range(tiles):
            encode(shard_of(event), t)

    lax.fori_loop(0, peers // 2, build_enc, 0)
    for k in z_order[:2]:
        relay(k)
    lax.fori_loop(peers // 2, peers, build_enc, 0)
    relay(0)
    for copy in par_copies:
        copy.wait()
    agg[...] = jnp.zeros_like(agg)
    for t in range(tiles):
        encode(me, t)
    for k in z_order[2:]:
        relay(k)
    for event in [0] + z_order:
        encode_event(event)
    early = peers // 2
    pieces = [early * i // (lines - 1) for i in range(lines)]
    for i, k in enumerate(z_order):
        lax.fori_loop(pieces[i], pieces[i + 1], build_dec, 0)
        relay(lines - 1 + k)
    for k in z_order:
        encode_event(lines - 1 + k)

    hidden = sum(
        jnp.dot(agg[h].astype(jnp.bfloat16), w_node_all[h], preferred_element_type=jnp.float32)
        for h in range(2)
    )
    width = hidden.shape[1] // 2
    projected = sum(
        jnp.dot(
            (
                embed_all[h].astype(jnp.float32) + silu(hidden[:, h * width : (h + 1) * width])
            ).astype(jnp.bfloat16),
            w_dec_all[h], preferred_element_type=jnp.float32,
        )
        for h in range(2)
    ).astype(jnp.bfloat16)
    for h in range(2):
        proj[h] = projected[:, h * cols : (h + 1) * cols]

    my_rows = pl.ds(pl.multiple_of(core * half_mesh, half_mesh), half_mesh)
    own_copy = pltpu.make_async_copy(proj.at[core], proj_all.at[me, my_rows], local_sem.at[0])
    own_copy.start()
    into = proj_all.at[me, my_rows]
    p_copies = []
    for flip in range(2):
        chan = (core + flip) % 2
        copy = remote(proj.at[chan], into, py_send.at[flip], py_recv.at[flip], other, chan)
        copy.start()
        p_copies.append(copy)
    for k in z_order:
        to = ((line + k) % lines) * 2 + side
        for flip in range(2):
            chan = (core + flip) % 2
            copy = remote(
                proj.at[chan], into, pz_send.at[k, flip], pz_recv.at[k, flip], to, chan
            )
            copy.start()
            p_copies.append(copy)
    mate_copy = remote(proj.at[mate], into, pm_send.at[0], pm_recv.at[0], me, mate)
    mate_copy.start()
    p_copies.append(mate_copy)

    def decode(shard):
        for t in range(2):
            rows = slice(t * half_grid, (t + 1) * half_grid)
            total[rows, :] += jnp.dot(
                dec[shard, rows, :], proj_all[shard], preferred_element_type=jnp.float32
            )

    pieces = [early + (peers - early) * i // (lines - 1) for i in range(lines)]
    r_copies = []
    for i, k in enumerate(z_order):
        lax.fori_loop(pieces[i], pieces[i + 1], build_dec, 0)
        shard = ((line + lines - k) % lines) * 2 + side
        for flip in range(2):
            remote(proj.at[core], into, pz_send.at[k, flip], pz_recv.at[k, flip], me, mate).wait_recv()
        copy = remote(
            proj_all.at[shard], proj_all.at[shard], pr_send.at[k], pr_recv.at[k], other, core
        )
        copy.start()
        r_copies.append(copy)
    own_cols = x_ref[:, pl.ds(pl.multiple_of(core * cols, cols), cols)]
    total[...] = own_cols.astype(jnp.float32)
    own_copy.wait()
    mate_copy.wait_recv()
    decode(me)
    for copy in p_copies[:2]:
        copy.wait_recv()
    decode(other)
    for k in z_order:
        decode(((line + lines - k) % lines) * 2 + side)
    for i, k in enumerate(z_order):
        r_copies[i].wait_recv()
        decode(((line + lines - k) % lines) * 2 + (1 - side))
    out_ref[...] = total[...].astype(jnp.bfloat16)

    for copy in y_copies + list(z_copies.values()) + list(mate_copies.values()) + p_copies + r_copies:
        copy.wait_send()


def fused(grid_state, w_src, bias_src, mesh_embed, w_node, w_dec, slot_src, slot_dst, slot_count):
    peers = lax.axis_size("graph")
    own_index = lax.axis_index("graph")
    capacity = slot_src.shape[2]
    positions = jnp.arange(capacity, dtype=jnp.int32)
    sent = lax.dynamic_slice_in_dim(slot_count, own_index, 1, 0)[0]
    received = lax.dynamic_slice_in_dim(slot_count, own_index, 1, 1)[:, 0]
    src = jnp.where(positions < sent[:, None], slot_src[0], -1)[:, None, :]
    dst = jnp.where(positions < received[:, None], slot_dst[:, 0, :], -1)[:, None, :]
    grid_rows, chans = grid_state.shape
    mesh_rows = mesh_embed.shape[0]
    hidden = w_src.shape[1]
    lines = peers // 2
    bf16, f32 = jnp.bfloat16, jnp.float32
    dma = pltpu.SemaphoreType.DMA
    vmem = pl.BlockSpec(memory_space=pltpu.VMEM)
    tile = grid_rows // 2
    return pl.pallas_call(
        functools.partial(graph_kernel, peers),
        out_shape=jax.ShapeDtypeStruct((grid_rows, chans // 2), bf16),
        in_specs=[vmem] * 8,
        out_specs=vmem,
        scratch_shapes=[
            pltpu.VMEM((peers, grid_rows, chans), bf16),
            pltpu.VMEM((peers, 1, capacity), jnp.int32),
            pltpu.VMEM((peers, 1, capacity), jnp.int32),
            pltpu.VMEM((2,) + w_src.shape, bf16),
            pltpu.VMEM((2, 1, hidden), f32),
            pltpu.VMEM((2, mesh_rows // 2, hidden), bf16),
            pltpu.VMEM((2,) + w_node.shape, bf16),
            pltpu.VMEM((2,) + w_dec.shape, bf16),
            pltpu.VMEM((peers, grid_rows // tile, mesh_rows // 2, tile), bf16),
            pltpu.VMEM((peers, grid_rows, mesh_rows), bf16),
            pltpu.VMEM((mesh_rows, capacity), bf16),
            pltpu.VMEM((2, mesh_rows // 2, hidden), f32),
            pltpu.VMEM((2, mesh_rows // 2, chans // 2), bf16),
            pltpu.VMEM((peers, mesh_rows, chans // 2), bf16),
            pltpu.VMEM((grid_rows, chans // 2), f32),
            dma((8,)), dma((5,)), dma((5,)), dma((2, peers)), dma((2, peers)),
            dma((lines,)), dma((lines,)), dma((peers,)), dma((peers,)), dma((peers,)),
            dma((lines, 2)), dma((lines, 2)), dma((2,)), dma((2,)), dma((1,)), dma((1,)),
            dma((lines,)), dma((lines,)),
        ],
        compiler_params=pltpu.CompilerParams(collective_id=0, has_side_effects=True),
    )(grid_state, w_src, bias_src[None, :], mesh_embed, w_node, w_dec, src, dst)


def held_bytes(peers, grid_state, mesh_embed, *rest):
    grid_rows, chans = grid_state.shape
    mesh_rows = mesh_embed.shape[0]
    return 2 * peers * grid_rows * (chans + 2 * mesh_rows)


def per_device(grid_state, w_src, bias_src, mesh_embed, *rest):
    peers = lax.axis_size("graph")
    fits = (
        peers % 2 == 0
        and peers >= 4
        and lax.axis_size("chan") == 2
        and held_bytes(peers, grid_state, mesh_embed) <= VMEM_BUDGET
    )
    body = fused if fits else on_device
    return body(grid_state, w_src, bias_src, mesh_embed, *rest)


def solution(mesh):
    placed = (
        P(("member", "graph"), None),
        P(None, "chan"),
        P("chan"),
        P("graph", "chan"),
        P("chan", None),
        P("chan", None),
        P("graph", None, None),
        P(None, "graph", None),
        P(),
    )
    return jax.shard_map(
        per_device,
        mesh=mesh,
        in_specs=placed,
        out_specs=P(("member", "graph"), "chan"),
        check_vma=False,
    )
```

```python
import functools
import math

import jax
import jax.numpy as jnp
from jax import lax
from jax.experimental import pallas as pl
from jax.experimental.pallas import tpu as pltpu
from jax.sharding import PartitionSpec as P

CHUNKS = 2
VMEM_BUDGET = 48 * 2**20
MESH = pl.DeviceIdType.MESH
NT = (((1,), (1,)), ((), ()))


def edge_network(source_rows, w_src, bias_src):
    return jax.nn.silu(
        jnp.dot(source_rows, w_src, preferred_element_type=jnp.float32) + bias_src
    ).astype(jnp.bfloat16)


def segment_rows(values, indices, usable, row_count):
    slot_total = values.shape[0]
    width = values.shape[1]
    block_len = math.gcd(slot_total, 2048)
    block_count = slot_total // block_len
    targets = jnp.where(usable, indices, -1).reshape(block_count, block_len)
    pieces = values.reshape(block_count, block_len, width)
    row_ids = jnp.arange(row_count, dtype=jnp.int32)

    def add_block(summed, scan_item):
        row_target, piece_vals = scan_item
        one_hot = (row_ids[:, None] == row_target[None, :]).astype(jnp.bfloat16)
        return (summed + jnp.dot(one_hot, piece_vals, preferred_element_type=jnp.float32), None)

    result, unused = lax.scan(
        add_block, jnp.zeros((row_count, width), jnp.float32), (targets, pieces)
    )
    return result


def on_device(
    grid_state, w_src, bias_src, mesh_embed, w_node, w_dec, slot_src, slot_dst, slot_count
):
    peers = lax.axis_size("graph")
    own_index = lax.axis_index("graph")
    core_index = lax.axis_index("chan")
    capacity = slot_src.shape[2]
    positions = jnp.arange(capacity, dtype=jnp.int32)
    grid_rows = grid_state.shape[0]
    mesh_rows = mesh_embed.shape[0]
    sent_counts = lax.dynamic_slice_in_dim(slot_count, own_index, 1, 0)[0]
    recv_counts = lax.dynamic_slice_in_dim(slot_count, own_index, 1, 1)[:, 0]
    half_slots = capacity // 2
    chosen = lax.dynamic_slice_in_dim(slot_src[0], core_index * half_slots, half_slots, 1)
    picked = jnp.take(grid_state, chosen.reshape(-1), axis=0).reshape(
        peers, half_slots, grid_state.shape[1]
    )
    arrived = lax.all_to_all(picked, "graph", split_axis=0, concat_axis=0, tiled=True)
    joined = lax.all_gather(arrived, "chan", axis=1, tiled=True)
    messages = edge_network(joined.reshape(peers * capacity, grid_state.shape[1]), w_src, bias_src)
    arrive_ok = (positions[None, :] < recv_counts[:, None]).reshape(-1)
    dst_rows = slot_dst[:, 0, :].reshape(-1)
    aggregate = segment_rows(messages, dst_rows, arrive_ok, mesh_rows)
    partial_hidden = jnp.dot(
        aggregate.astype(jnp.bfloat16), w_node, preferred_element_type=jnp.float32
    )
    hidden_pre = lax.psum_scatter(partial_hidden, "chan", scatter_dimension=1, tiled=True)
    latent = (mesh_embed.astype(jnp.float32) + jax.nn.silu(hidden_pre)).astype(jnp.bfloat16)
    partial_proj = jnp.dot(latent, w_dec, preferred_element_type=jnp.float32)
    projected = lax.psum_scatter(partial_proj, "chan", scatter_dimension=1, tiled=True).astype(
        jnp.bfloat16
    )
    returned = jnp.take(projected, dst_rows, axis=0).reshape(peers, capacity, projected.shape[1])
    came_back = lax.all_to_all(returned, "graph", split_axis=0, concat_axis=0, tiled=True).reshape(
        peers * capacity, projected.shape[1]
    )
    send_ok = (positions[None, :] < sent_counts[:, None]).reshape(-1)
    decoded = segment_rows(came_back, slot_src[0].reshape(-1), send_ok, grid_rows)
    width_half = decoded.shape[1]
    own_cols = lax.dynamic_slice_in_dim(grid_state, core_index * width_half, width_half, 1)
    return (own_cols.astype(jnp.float32) + decoded).astype(jnp.bfloat16)


def silu(v):
    half = 0.5 * v
    return half + half * jnp.tanh(half)


def one_hot(first, rows, indices):
    row_ids = lax.broadcasted_iota(jnp.int32, (rows, indices.shape[1]), 0) + first
    return jnp.where(row_ids == indices, 1.0, 0.0).astype(jnp.bfloat16)


def graph_kernel(
    peers,
    x_ref, w_src_ref, bias_ref, embed_ref, w_node_ref, w_dec_ref, src_ref, dst_ref, count_ref,
    out_ref,
    x_all, src_own, src_in, dst_in, w_src_all, bias_all, embed_all, w_node_all, w_dec_all,
    enc, dec, hot, agg, proj, proj_all, total,
    local_sem, par_send, par_recv, idx_send, idx_recv,
    xo_send, xz_send, xy_send, x_recv, xm_send, xm_recv,
    po_send, pz_send, py_send, p_recv, pm_send, pm_recv,
):
    lines = peers // 2
    me = lax.axis_index("graph")
    core = lax.axis_index("chan")
    mate = 1 - core
    line, side = me // 2, me % 2
    other = line * 2 + (1 - side)
    grid_rows, chans = x_ref.shape
    half_grid = grid_rows // 2
    piece = half_grid // CHUNKS
    mesh_rows = embed_ref.shape[0]
    half_mesh = mesh_rows // 2
    cols = chans // 2
    tile = enc.shape[3]
    tiles = grid_rows // tile
    capacity = src_ref.shape[2]

    def remote(src, dst, send, recv, graph, chan):
        return pltpu.make_async_remote_copy(
            src_ref=src, dst_ref=dst, send_sem=send, recv_sem=recv,
            device_id={"graph": graph, "chan": chan}, device_id_type=MESH,
        )

    barrier = pltpu.get_barrier_semaphore()
    for step in range(peers):
        for chan in range(2):
            if step == 0 and chan == 0:
                continue
            pl.semaphore_signal(
                barrier, inc=1,
                device_id={"graph": (me + step) % peers, "chan": (core + chan) % 2},
                device_id_type=MESH,
            )
    slots = lax.broadcasted_iota(jnp.int32, (1, capacity), 1)
    for to in range(peers):
        src_own[to] = jnp.where(slots < count_ref[me, to], src_ref[0, to : to + 1, :], -1)
    my_rows = pl.ds(pl.multiple_of(core * half_mesh, half_mesh), half_mesh)
    mate_rows = pl.ds(pl.multiple_of(mate * half_mesh, half_mesh), half_mesh)
    locals_ = [
        pltpu.make_async_copy(x_ref, x_all.at[me], local_sem.at[0]),
        pltpu.make_async_copy(w_src_ref, w_src_all.at[core], local_sem.at[1]),
        pltpu.make_async_copy(bias_ref, bias_all.at[core], local_sem.at[2]),
        pltpu.make_async_copy(embed_ref.at[my_rows], embed_all.at[core], local_sem.at[3]),
        pltpu.make_async_copy(w_node_ref, w_node_all.at[core], local_sem.at[4]),
        pltpu.make_async_copy(w_dec_ref, w_dec_all.at[core], local_sem.at[5]),
        pltpu.make_async_copy(src_own.at[me], src_in.at[me], local_sem.at[6]),
        pltpu.make_async_copy(dst_ref.at[me], dst_in.at[me], local_sem.at[7]),
    ]
    for copy in locals_:
        copy.start()
    pl.semaphore_wait(barrier, 2 * peers - 1)

    sends = []
    idx_copies = []
    for step in range(1, peers):
        to = (me + step) % peers
        for at, (ref, into) in enumerate(((src_own, src_in), (dst_ref, dst_in))):
            copy = remote(
                ref.at[to], into.at[me], idx_send.at[at, step], idx_recv.at[at, step], to, core
            )
            copy.start()
            idx_copies.append(copy)

    def nearest(at):
        return sorted((p for p in range(lines) if p != at), key=lambda p: (abs(p - at), p))

    from_line = [
        sum(jnp.where(line == at, nearest(at)[i], 0) for at in range(lines))
        for i in range(lines - 1)
    ]
    up, down = (line + 1) * 2 + side, (line - 1) * 2 + side

    def along(source, make):
        for going, target in (
            ((source <= line) & (line < lines - 1), up),
            ((source >= line) & (line > 0), down),
        ):
            @pl.when(going)
            def _(target=target):
                make(target).start()
            sends.append((going, functools.partial(make, target)))

    def begin(copy):
        copy.start()
        sends.append((None, lambda: copy))

    def x_part(shard, half, c):
        first = pl.multiple_of(half * half_grid, half_grid) + c * piece
        return x_all.at[shard, pl.ds(pl.multiple_of(first, piece), piece)]

    def x_own(c):
        first = pl.multiple_of(core * half_grid, half_grid) + c * piece
        return x_ref.at[pl.ds(pl.multiple_of(first, piece), piece)]

    for c in range(CHUNKS):
        begin(remote(x_own(c), x_part(me, core, c), xy_send.at[line, c], x_recv.at[1, line, c], other, core))
        for at, (going, target) in enumerate(((line < lines - 1, up), (line > 0, down))):
            def make(c=c, at=at, target=target):
                return remote(
                    x_own(c), x_part(me, core, c), xo_send.at[at, c], x_recv.at[0, line, c],
                    target, core,
                )
            @pl.when(going)
            def _(make=make):
                make().start()
            sends.append((going, make))

    par_copies = [
        remote(w_src_ref, w_src_all.at[core], par_send.at[0], par_recv.at[0], me, mate),
        remote(bias_ref, bias_all.at[core], par_send.at[1], par_recv.at[1], me, mate),
        remote(embed_ref.at[mate_rows], embed_all.at[core], par_send.at[2], par_recv.at[2], me, mate),
        remote(w_node_ref, w_node_all.at[core], par_send.at[3], par_recv.at[3], me, mate),
        remote(w_dec_ref, w_dec_all.at[core], par_send.at[4], par_recv.at[4], me, mate),
    ]
    for copy in par_copies:
        copy.start()

    def to_mate(flip, source, c, shard):
        ref = x_part(shard, core, c)
        begin(remote(ref, ref, xm_send.at[flip, source, c], xm_recv.at[flip, source, c], me, mate))

    def relay(i, c):
        source = from_line[i]
        shard = source * 2 + side
        ref = x_part(shard, core, c)
        remote(ref, ref, xz_send.at[source, c], x_recv.at[0, source, c], me, mate).wait_recv()
        along(source, lambda target: remote(
            ref, ref, xz_send.at[source, c], x_recv.at[0, source, c], target, core))
        begin(remote(ref, ref, xy_send.at[source, c], x_recv.at[1, source, c], other, core))
        to_mate(0, source, c, shard)

    def take(source, c):
        shard = source * 2 + (1 - side)
        ref = x_part(shard, core, c)
        remote(ref, ref, xz_send.at[source, c], x_recv.at[1, source, c], me, mate).wait_recv()
        to_mate(1, source, c, shard)

    def build_enc(shard, carry):
        hot[: half_mesh, :] = one_hot(core * half_mesh, half_mesh, dst_ref[shard])
        for t in range(tiles):
            picks = one_hot(t * tile, tile, src_in[shard])
            enc[shard, t] = lax.dot_general(
                hot[: half_mesh, :], picks, NT, preferred_element_type=jnp.float32
            ).astype(jnp.bfloat16)
        return carry

    def build_dec(shard, carry):
        hot[...] = one_hot(0, mesh_rows, dst_in[shard])
        for t in range(grid_rows // 256):
            picks = one_hot(t * 256, 256, src_own[shard])
            dec[shard, t * 256 : (t + 1) * 256, :] = lax.dot_general(
                picks, hot[...], NT, preferred_element_type=jnp.float32
            ).astype(jnp.bfloat16)
        return carry

    done = {build_enc: 0, build_dec: 0}

    def build(which, count):
        first = done[which]
        last = min(first + count, peers)
        if last > first:
            lax.fori_loop(first, last, which, 0)
        done[which] = last

    def encode(shard):
        def step(t, carry):
            rows = pl.ds(pl.multiple_of(t * tile, tile), tile)
            for h in range(2):
                pre = jnp.dot(
                    x_all[shard, rows, :], w_src_all[h], preferred_element_type=jnp.float32
                ) + bias_all[h]
                agg[h] += jnp.dot(
                    enc[shard, t], silu(pre).astype(jnp.bfloat16),
                    preferred_element_type=jnp.float32,
                )
            return carry
        lax.fori_loop(0, tiles, step, 0)

    def encode_from(flip, source):
        shard = source * 2 + (side if flip == 0 else 1 - side)
        for c in range(CHUNKS):
            ref = x_part(shard, mate, c)
            remote(ref, ref, xm_send.at[flip, source, c], xm_recv.at[flip, source, c], me, mate).wait_recv()
        encode(shard)

    for copy in locals_:
        copy.wait()
    for copy in idx_copies:
        copy.wait()
    agg[...] = jnp.zeros_like(agg)
    total[...] = x_ref[:, pl.ds(pl.multiple_of(core * cols, cols), cols)].astype(jnp.float32)
    build(build_enc, peers * 3 // 8)
    last = lines - 2
    for i in range(lines - 1):
        for c in range(CHUNKS):
            relay(i, c)
            if i == 0:
                build(build_enc, peers // CHUNKS // 4)
            else:
                take(from_line[i - 1], c)
                if c < CHUNKS - 1:
                    build(build_dec, 1)
        if i == 0:
            for c in range(CHUNKS):
                take(line, c)
            for copy in par_copies:
                copy.wait()
            build(build_enc, peers)
            encode(me)
        elif i == 1:
            encode_from(0, from_line[0])
            encode_from(1, line)
            build(build_dec, 1)
        else:
            encode_from(0, from_line[i - 1])
            encode_from(1, from_line[i - 2])
            build(build_dec, 1)
    encode_from(0, from_line[last])
    encode_from(1, from_line[last - 1])
    for c in range(CHUNKS):
        take(from_line[last], c)
    encode_from(1, from_line[last])

    hidden = sum(
        jnp.dot(agg[h].astype(jnp.bfloat16), w_node_all[h], preferred_element_type=jnp.float32)
        for h in range(2)
    )
    width = hidden.shape[1] // 2
    projected = sum(
        jnp.dot(
            (
                embed_all[h].astype(jnp.float32) + silu(hidden[:, h * width : (h + 1) * width])
            ).astype(jnp.bfloat16),
            w_dec_all[h], preferred_element_type=jnp.float32,
        )
        for h in range(2)
    ).astype(jnp.bfloat16)
    for h in range(2):
        proj[h] = projected[:, h * cols : (h + 1) * cols]

    own_copy = pltpu.make_async_copy(proj.at[core], proj_all.at[me, my_rows], local_sem.at[0])
    own_copy.start()
    into = proj_all.at[me, my_rows]
    for flip in range(2):
        chan = (core + flip) % 2
        begin(remote(proj.at[chan], into, py_send.at[line, flip], p_recv.at[1, line, core], other, chan))
        for at, (going, target) in enumerate(((line < lines - 1, up), (line > 0, down))):
            def make(flip=flip, chan=chan, at=at, target=target):
                return remote(
                    proj.at[chan], into, po_send.at[at, flip], p_recv.at[0, line, core],
                    target, chan,
                )
            @pl.when(going)
            def _(make=make):
                make().start()
            sends.append((going, make))
    begin(remote(proj.at[mate], into, pm_send.at[0], pm_recv.at[0], me, mate))

    def p_part(shard, half):
        return proj_all.at[shard, half * half_mesh : (half + 1) * half_mesh]

    def p_wait(flip, source, half):
        ref = p_part(source * 2 + (side if flip == 0 else 1 - side), half)
        remote(ref, ref, pz_send.at[source, half], p_recv.at[flip, source, half], me, mate).wait_recv()

    def p_relay(i):
        source = from_line[i]
        for half in range(2):
            p_wait(0, source, half)
            ref = p_part(source * 2 + side, half)
            along(source, lambda target, half=half, ref=ref: remote(
                ref, ref, pz_send.at[source, half], p_recv.at[0, source, half], target, core))
            begin(remote(ref, ref, py_send.at[source, half], p_recv.at[1, source, half], other, core))

    def decode(shard):
        def step(t, carry):
            rows = pl.ds(pl.multiple_of(t * half_grid, half_grid), half_grid)
            total[rows, :] += jnp.dot(
                dec[shard, rows, :], proj_all[shard], preferred_element_type=jnp.float32
            )
            return carry
        lax.fori_loop(0, 2, step, 0)

    left = peers - done[build_dec]
    for i in range(lines - 1):
        build(build_dec, -(-left // (lines - 1)))
        p_relay(i)
    own_copy.wait()
    remote(proj.at[mate], into, pm_send.at[0], pm_recv.at[0], me, mate).wait_recv()
    decode(me)
    for i in range(lines - 1):
        decode(from_line[i] * 2 + side)
    for source in [line] + from_line:
        for half in range(2):
            p_wait(1, source, half)
        decode(source * 2 + 1 - side)
    out_ref[...] = total[...].astype(jnp.bfloat16)

    for going, make in sends:
        if going is None:
            make().wait_send()
        else:
            @pl.when(going)
            def _(make=make):
                make().wait_send()


def fused(grid_state, w_src, bias_src, mesh_embed, w_node, w_dec, slot_src, slot_dst, slot_count):
    peers = lax.axis_size("graph")
    capacity = slot_src.shape[2]
    grid_rows, chans = grid_state.shape
    mesh_rows = mesh_embed.shape[0]
    hidden = w_src.shape[1]
    lines = peers // 2
    bf16, f32 = jnp.bfloat16, jnp.float32
    dma = pltpu.SemaphoreType.DMA
    vmem = pl.BlockSpec(memory_space=pltpu.VMEM)
    tile = grid_rows // 2
    return pl.pallas_call(
        functools.partial(graph_kernel, peers),
        out_shape=jax.ShapeDtypeStruct((grid_rows, chans // 2), bf16),
        in_specs=[vmem] * 8 + [pl.BlockSpec(memory_space=pltpu.SMEM)],
        out_specs=vmem,
        scratch_shapes=[
            pltpu.VMEM((peers, grid_rows, chans), bf16),
            pltpu.VMEM((peers, 1, capacity), jnp.int32),
            pltpu.VMEM((peers, 1, capacity), jnp.int32),
            pltpu.VMEM((peers, 1, capacity), jnp.int32),
            pltpu.VMEM((2,) + w_src.shape, bf16),
            pltpu.VMEM((2, 1, hidden), f32),
            pltpu.VMEM((2, mesh_rows // 2, hidden), bf16),
            pltpu.VMEM((2,) + w_node.shape, bf16),
            pltpu.VMEM((2,) + w_dec.shape, bf16),
            pltpu.VMEM((peers, grid_rows // tile, mesh_rows // 2, tile), bf16),
            pltpu.VMEM((peers, grid_rows, mesh_rows), bf16),
            pltpu.VMEM((mesh_rows, capacity), bf16),
            pltpu.VMEM((2, mesh_rows // 2, hidden), f32),
            pltpu.VMEM((2, mesh_rows // 2, chans // 2), bf16),
            pltpu.VMEM((peers, mesh_rows, chans // 2), bf16),
            pltpu.VMEM((grid_rows, chans // 2), f32),
            dma((8,)), dma((5,)), dma((5,)), dma((2, peers)), dma((2, peers)),
            dma((2, CHUNKS)), dma((lines, CHUNKS)), dma((lines, CHUNKS)), dma((2, lines, CHUNKS)),
            dma((2, lines, CHUNKS)), dma((2, lines, CHUNKS)),
            dma((2, 2)), dma((lines, 2)), dma((lines, 2)), dma((2, lines, 2)), dma((1,)), dma((1,)),
        ],
        compiler_params=pltpu.CompilerParams(collective_id=0, has_side_effects=True),
    )(grid_state, w_src, bias_src[None, :], mesh_embed, w_node, w_dec, slot_src, slot_dst, slot_count)


def held_bytes(peers, grid_state, mesh_embed, *rest):
    grid_rows, chans = grid_state.shape
    mesh_rows = mesh_embed.shape[0]
    return 2 * peers * grid_rows * (chans + 2 * mesh_rows)


def per_device(grid_state, w_src, bias_src, mesh_embed, *rest):
    peers = lax.axis_size("graph")
    fits = (
        peers % 2 == 0
        and peers >= 4
        and lax.axis_size("chan") == 2
        and held_bytes(peers, grid_state, mesh_embed) <= VMEM_BUDGET
    )
    body = fused if fits else on_device
    return body(grid_state, w_src, bias_src, mesh_embed, *rest)


def solution(mesh):
    placed = (
        P(("member", "graph"), None),
        P(None, "chan"),
        P("chan"),
        P("graph", "chan"),
        P("chan", None),
        P("chan", None),
        P("graph", None, None),
        P(None, "graph", None),
        P(),
    )
    return jax.shard_map(
        per_device,
        mesh=mesh,
        in_specs=placed,
        out_specs=P(("member", "graph"), "chan"),
        check_vma=False,
    )
```

```python
import functools
import math

import jax
import jax.numpy as jnp
from jax import lax
from jax.experimental import pallas as pl
from jax.experimental.pallas import tpu as pltpu
from jax.sharding import PartitionSpec as P

CHUNKS = 2
HOT = jnp.float8_e4m3fn
VMEM_BUDGET = 48 * 2**20
MESH = pl.DeviceIdType.MESH
NT = (((1,), (1,)), ((), ()))


def edge_network(source_rows, w_src, bias_src):
    return jax.nn.silu(
        jnp.dot(source_rows, w_src, preferred_element_type=jnp.float32) + bias_src
    ).astype(jnp.bfloat16)


def segment_rows(values, indices, usable, row_count):
    slot_total = values.shape[0]
    width = values.shape[1]
    block_len = math.gcd(slot_total, 2048)
    block_count = slot_total // block_len
    targets = jnp.where(usable, indices, -1).reshape(block_count, block_len)
    pieces = values.reshape(block_count, block_len, width)
    row_ids = jnp.arange(row_count, dtype=jnp.int32)

    def add_block(summed, scan_item):
        row_target, piece_vals = scan_item
        one_hot = (row_ids[:, None] == row_target[None, :]).astype(jnp.bfloat16)
        return (summed + jnp.dot(one_hot, piece_vals, preferred_element_type=jnp.float32), None)

    result, unused = lax.scan(
        add_block, jnp.zeros((row_count, width), jnp.float32), (targets, pieces)
    )
    return result


def on_device(
    grid_state, w_src, bias_src, mesh_embed, w_node, w_dec, slot_src, slot_dst, slot_count
):
    peers = lax.axis_size("graph")
    own_index = lax.axis_index("graph")
    core_index = lax.axis_index("chan")
    capacity = slot_src.shape[2]
    positions = jnp.arange(capacity, dtype=jnp.int32)
    grid_rows = grid_state.shape[0]
    mesh_rows = mesh_embed.shape[0]
    sent_counts = lax.dynamic_slice_in_dim(slot_count, own_index, 1, 0)[0]
    recv_counts = lax.dynamic_slice_in_dim(slot_count, own_index, 1, 1)[:, 0]
    half_slots = capacity // 2
    chosen = lax.dynamic_slice_in_dim(slot_src[0], core_index * half_slots, half_slots, 1)
    picked = jnp.take(grid_state, chosen.reshape(-1), axis=0).reshape(
        peers, half_slots, grid_state.shape[1]
    )
    arrived = lax.all_to_all(picked, "graph", split_axis=0, concat_axis=0, tiled=True)
    joined = lax.all_gather(arrived, "chan", axis=1, tiled=True)
    messages = edge_network(joined.reshape(peers * capacity, grid_state.shape[1]), w_src, bias_src)
    arrive_ok = (positions[None, :] < recv_counts[:, None]).reshape(-1)
    dst_rows = slot_dst[:, 0, :].reshape(-1)
    aggregate = segment_rows(messages, dst_rows, arrive_ok, mesh_rows)
    partial_hidden = jnp.dot(
        aggregate.astype(jnp.bfloat16), w_node, preferred_element_type=jnp.float32
    )
    hidden_pre = lax.psum_scatter(partial_hidden, "chan", scatter_dimension=1, tiled=True)
    latent = (mesh_embed.astype(jnp.float32) + jax.nn.silu(hidden_pre)).astype(jnp.bfloat16)
    partial_proj = jnp.dot(latent, w_dec, preferred_element_type=jnp.float32)
    projected = lax.psum_scatter(partial_proj, "chan", scatter_dimension=1, tiled=True).astype(
        jnp.bfloat16
    )
    returned = jnp.take(projected, dst_rows, axis=0).reshape(peers, capacity, projected.shape[1])
    came_back = lax.all_to_all(returned, "graph", split_axis=0, concat_axis=0, tiled=True).reshape(
        peers * capacity, projected.shape[1]
    )
    send_ok = (positions[None, :] < sent_counts[:, None]).reshape(-1)
    decoded = segment_rows(came_back, slot_src[0].reshape(-1), send_ok, grid_rows)
    width_half = decoded.shape[1]
    own_cols = lax.dynamic_slice_in_dim(grid_state, core_index * width_half, width_half, 1)
    return (own_cols.astype(jnp.float32) + decoded).astype(jnp.bfloat16)


def silu(v):
    half = 0.5 * v
    return half + half * jnp.tanh(half)


def one_hot(first, rows, indices):
    row_ids = lax.broadcasted_iota(jnp.int32, (rows, indices.shape[1]), 0) + first
    return jnp.where(row_ids == indices, 1.0, 0.0).astype(HOT)


def graph_kernel(
    peers,
    x_ref, w_src_ref, bias_ref, embed_ref, w_node_ref, w_dec_ref, src_ref, dst_ref, count_ref,
    out_ref,
    x_all, src_own, src_in, dst_in, w_src_all, bias_all, embed_all, w_node_all, w_dec_all,
    enc, dec, hot, agg, proj, proj_all, total,
    local_sem, par_send, par_recv, idx_send, idx_recv,
    xo_send, xz_send, xy_send, x_recv, xm_send, xm_recv,
    po_send, pz_send, py_send, p_recv, pm_send, pm_recv, dec_send, dec_recv,
):
    lines = peers // 2
    me = lax.axis_index("graph")
    core = lax.axis_index("chan")
    mate = 1 - core
    line, side = me // 2, me % 2
    other = line * 2 + (1 - side)
    grid_rows, chans = x_ref.shape
    half_grid = grid_rows // 2
    piece = half_grid // CHUNKS
    mesh_rows = embed_ref.shape[0]
    half_mesh = mesh_rows // 2
    cols = chans // 2
    tile = enc.shape[3]
    tiles = grid_rows // tile
    capacity = src_ref.shape[2]

    def remote(src, dst, send, recv, graph, chan):
        return pltpu.make_async_remote_copy(
            src_ref=src, dst_ref=dst, send_sem=send, recv_sem=recv,
            device_id={"graph": graph, "chan": chan}, device_id_type=MESH,
        )

    barrier = pltpu.get_barrier_semaphore()
    for step in range(peers):
        for chan in range(2):
            if step == 0 and chan == 0:
                continue
            pl.semaphore_signal(
                barrier, inc=1,
                device_id={"graph": (me + step) % peers, "chan": (core + chan) % 2},
                device_id_type=MESH,
            )
    slots = lax.broadcasted_iota(jnp.int32, (1, capacity), 1)
    for to in range(peers):
        src_own[to] = jnp.where(slots < count_ref[me, to], src_ref[0, to : to + 1, :], -1)
    my_rows = pl.ds(pl.multiple_of(core * half_mesh, half_mesh), half_mesh)
    mate_rows = pl.ds(pl.multiple_of(mate * half_mesh, half_mesh), half_mesh)
    locals_ = [
        pltpu.make_async_copy(x_ref, x_all.at[me], local_sem.at[0]),
        pltpu.make_async_copy(w_src_ref, w_src_all.at[core], local_sem.at[1]),
        pltpu.make_async_copy(bias_ref, bias_all.at[core], local_sem.at[2]),
        pltpu.make_async_copy(embed_ref.at[my_rows], embed_all.at[core], local_sem.at[3]),
        pltpu.make_async_copy(w_node_ref, w_node_all.at[core], local_sem.at[4]),
        pltpu.make_async_copy(w_dec_ref, w_dec_all.at[core], local_sem.at[5]),
        pltpu.make_async_copy(src_own.at[me], src_in.at[me], local_sem.at[6]),
        pltpu.make_async_copy(dst_ref.at[me], dst_in.at[me], local_sem.at[7]),
    ]
    for copy in locals_:
        copy.start()
    pl.semaphore_wait(barrier, 2 * peers - 1)

    sends = []
    idx_copies = []
    for step in range(1, peers):
        to = (me + step) % peers
        for at, (ref, into) in enumerate(((src_own, src_in), (dst_ref, dst_in))):
            copy = remote(
                ref.at[to], into.at[me], idx_send.at[at, step], idx_recv.at[at, step], to, core
            )
            copy.start()
            idx_copies.append(copy)

    def nearest(at):
        return sorted((p for p in range(lines) if p != at), key=lambda p: (abs(p - at), p))

    from_line = [
        sum(jnp.where(line == at, nearest(at)[i], 0) for at in range(lines))
        for i in range(lines - 1)
    ]
    up, down = (line + 1) * 2 + side, (line - 1) * 2 + side

    def along(source, make):
        for going, target in (
            ((source <= line) & (line < lines - 1), up),
            ((source >= line) & (line > 0), down),
        ):
            @pl.when(going)
            def _(target=target):
                make(target).start()
            sends.append((going, functools.partial(make, target)))

    def begin(copy):
        copy.start()
        sends.append((None, lambda: copy))

    def x_part(shard, half, c):
        first = pl.multiple_of(half * half_grid, half_grid) + c * piece
        return x_all.at[shard, pl.ds(pl.multiple_of(first, piece), piece)]

    def x_own(c):
        first = pl.multiple_of(core * half_grid, half_grid) + c * piece
        return x_ref.at[pl.ds(pl.multiple_of(first, piece), piece)]

    for c in range(CHUNKS):
        begin(remote(x_own(c), x_part(me, core, c), xy_send.at[line, c], x_recv.at[1, line, c], other, core))
        for at, (going, target) in enumerate(((line < lines - 1, up), (line > 0, down))):
            def make(c=c, at=at, target=target):
                return remote(
                    x_own(c), x_part(me, core, c), xo_send.at[at, c], x_recv.at[0, line, c],
                    target, core,
                )
            @pl.when(going)
            def _(make=make):
                make().start()
            sends.append((going, make))

    par_copies = [
        remote(w_src_ref, w_src_all.at[core], par_send.at[0], par_recv.at[0], me, mate),
        remote(bias_ref, bias_all.at[core], par_send.at[1], par_recv.at[1], me, mate),
        remote(embed_ref.at[mate_rows], embed_all.at[core], par_send.at[2], par_recv.at[2], me, mate),
        remote(w_node_ref, w_node_all.at[core], par_send.at[3], par_recv.at[3], me, mate),
        remote(w_dec_ref, w_dec_all.at[core], par_send.at[4], par_recv.at[4], me, mate),
    ]
    for copy in par_copies:
        copy.start()

    def to_mate(flip, source, c, shard):
        ref = x_part(shard, core, c)
        begin(remote(ref, ref, xm_send.at[flip, source, c], xm_recv.at[flip, source, c], me, mate))

    def relay(i, c):
        source = from_line[i]
        shard = source * 2 + side
        ref = x_part(shard, core, c)
        remote(ref, ref, xz_send.at[source, c], x_recv.at[0, source, c], me, mate).wait_recv()
        along(source, lambda target: remote(
            ref, ref, xz_send.at[source, c], x_recv.at[0, source, c], target, core))
        begin(remote(ref, ref, xy_send.at[source, c], x_recv.at[1, source, c], other, core))
        to_mate(0, source, c, shard)

    def take(source, c):
        shard = source * 2 + (1 - side)
        ref = x_part(shard, core, c)
        remote(ref, ref, xz_send.at[source, c], x_recv.at[1, source, c], me, mate).wait_recv()
        to_mate(1, source, c, shard)

    def build_enc(i, carry):
        shard = (me + i) % peers
        hot[: half_mesh, :] = one_hot(core * half_mesh, half_mesh, dst_ref[shard])
        for t in range(tiles):
            picks = one_hot(t * tile, tile, src_in[shard])
            enc[shard, t] = lax.dot_general(
                hot[: half_mesh, :], picks, NT, preferred_element_type=jnp.float32
            ).astype(jnp.bfloat16)
        return carry

    def build_dec(i, carry):
        shard = (me + i) % peers
        hot[...] = one_hot(0, mesh_rows, dst_in[shard])
        for t in range(half_grid // 256):
            first = pl.multiple_of(core * half_grid, half_grid) + t * 256
            picks = one_hot(first, 256, src_own[shard])
            dec[shard, pl.ds(pl.multiple_of(first, 256), 256), :] = lax.dot_general(
                picks, hot[...], NT, preferred_element_type=jnp.float32
            ).astype(jnp.bfloat16)
        return carry

    done = {build_enc: 0, build_dec: 0}
    pending = []

    def dec_copy(i, half):
        shard = (me + i) % peers
        ref = dec.at[shard, pl.ds(pl.multiple_of(half * half_grid, half_grid), half_grid)]
        return remote(ref, ref, dec_send.at[shard], dec_recv.at[shard], me, mate)

    def flush():
        while pending:
            begin(dec_copy(pending.pop(0), core))

    def build(which, count):
        first = done[which]
        last = min(first + count, peers)
        if last > first:
            flush()
            lax.fori_loop(first, last, which, 0)
            if which is build_dec:
                pending.extend(range(first, last))
        done[which] = last

    def encode(shard):
        def step(t, carry):
            rows = pl.ds(pl.multiple_of(t * tile, tile), tile)
            for h in range(2):
                pre = jnp.dot(
                    x_all[shard, rows, :], w_src_all[h], preferred_element_type=jnp.float32
                ) + bias_all[h]
                agg[h] += jnp.dot(
                    enc[shard, t], silu(pre).astype(jnp.bfloat16),
                    preferred_element_type=jnp.float32,
                )
            return carry
        lax.fori_loop(0, tiles, step, 0)

    def encode_from(flip, source):
        shard = source * 2 + (side if flip == 0 else 1 - side)
        for c in range(CHUNKS):
            ref = x_part(shard, mate, c)
            remote(ref, ref, xm_send.at[flip, source, c], xm_recv.at[flip, source, c], me, mate).wait_recv()
        encode(shard)

    for copy in locals_:
        copy.wait()
    agg[...] = jnp.zeros_like(agg)
    total[...] = x_ref[:, pl.ds(pl.multiple_of(core * cols, cols), cols)].astype(jnp.float32)
    build(build_enc, 1)
    build(build_dec, 1)
    for copy in par_copies:
        copy.wait()
    encode(me)
    for copy in idx_copies:
        copy.wait()
    flush()
    build(build_enc, peers // 4)
    last = lines - 2
    for i in range(lines - 1):
        for c in range(CHUNKS):
            relay(i, c)
            if i == 0:
                build(build_enc, peers // CHUNKS // 4)
            else:
                take(from_line[i - 1], c)
                if c < CHUNKS - 1:
                    build(build_dec, 1)
        if i == 0:
            for c in range(CHUNKS):
                take(line, c)
            build(build_enc, peers)
        elif i == 1:
            encode_from(0, from_line[0])
            encode_from(1, line)
            build(build_dec, 1)
        else:
            encode_from(0, from_line[i - 1])
            encode_from(1, from_line[i - 2])
            build(build_dec, 1)
    encode_from(0, from_line[last])
    encode_from(1, from_line[last - 1])
    for c in range(CHUNKS):
        take(from_line[last], c)
    encode_from(1, from_line[last])

    hidden = sum(
        jnp.dot(agg[h].astype(jnp.bfloat16), w_node_all[h], preferred_element_type=jnp.float32)
        for h in range(2)
    )
    width = hidden.shape[1] // 2
    projected = sum(
        jnp.dot(
            (
                embed_all[h].astype(jnp.float32) + silu(hidden[:, h * width : (h + 1) * width])
            ).astype(jnp.bfloat16),
            w_dec_all[h], preferred_element_type=jnp.float32,
        )
        for h in range(2)
    ).astype(jnp.bfloat16)
    for h in range(2):
        proj[h] = projected[:, h * cols : (h + 1) * cols]

    own_copy = pltpu.make_async_copy(proj.at[core], proj_all.at[me, my_rows], local_sem.at[0])
    own_copy.start()
    into = proj_all.at[me, my_rows]
    for flip in range(2):
        chan = (core + flip) % 2
        begin(remote(proj.at[chan], into, py_send.at[line, flip], p_recv.at[1, line, core], other, chan))
        for at, (going, target) in enumerate(((line < lines - 1, up), (line > 0, down))):
            def make(flip=flip, chan=chan, at=at, target=target):
                return remote(
                    proj.at[chan], into, po_send.at[at, flip], p_recv.at[0, line, core],
                    target, chan,
                )
            @pl.when(going)
            def _(make=make):
                make().start()
            sends.append((going, make))
    begin(remote(proj.at[mate], into, pm_send.at[0], pm_recv.at[0], me, mate))

    def p_part(shard, half):
        return proj_all.at[shard, half * half_mesh : (half + 1) * half_mesh]

    def p_wait(flip, source, half):
        ref = p_part(source * 2 + (side if flip == 0 else 1 - side), half)
        remote(ref, ref, pz_send.at[source, half], p_recv.at[flip, source, half], me, mate).wait_recv()

    def p_relay(i):
        source = from_line[i]
        for half in range(2):
            p_wait(0, source, half)
            ref = p_part(source * 2 + side, half)
            along(source, lambda target, half=half, ref=ref: remote(
                ref, ref, pz_send.at[source, half], p_recv.at[0, source, half], target, core))
            begin(remote(ref, ref, py_send.at[source, half], p_recv.at[1, source, half], other, core))

    def decode(shard):
        def step(t, carry):
            rows = pl.ds(pl.multiple_of(t * half_grid, half_grid), half_grid)
            total[rows, :] += jnp.dot(
                dec[shard, rows, :], proj_all[shard], preferred_element_type=jnp.float32
            )
            return carry
        lax.fori_loop(0, 2, step, 0)

    flush()
    left = peers - done[build_dec]
    for i in range(lines - 1):
        build(build_dec, -(-left // (lines - 1)))
        p_relay(i)
    flush()
    for i in range(peers):
        dec_copy(i, mate).wait_recv()
    own_copy.wait()
    remote(proj.at[mate], into, pm_send.at[0], pm_recv.at[0], me, mate).wait_recv()
    decode(me)
    for i in range(lines - 1):
        decode(from_line[i] * 2 + side)
    for source in [line] + from_line:
        for half in range(2):
            p_wait(1, source, half)
        decode(source * 2 + 1 - side)
    out_ref[...] = total[...].astype(jnp.bfloat16)

    for going, make in sends:
        if going is None:
            make().wait_send()
        else:
            @pl.when(going)
            def _(make=make):
                make().wait_send()


def fused(grid_state, w_src, bias_src, mesh_embed, w_node, w_dec, slot_src, slot_dst, slot_count):
    peers = lax.axis_size("graph")
    capacity = slot_src.shape[2]
    grid_rows, chans = grid_state.shape
    mesh_rows = mesh_embed.shape[0]
    hidden = w_src.shape[1]
    lines = peers // 2
    bf16, f32 = jnp.bfloat16, jnp.float32
    dma = pltpu.SemaphoreType.DMA
    vmem = pl.BlockSpec(memory_space=pltpu.VMEM)
    tile = grid_rows // 2
    return pl.pallas_call(
        functools.partial(graph_kernel, peers),
        out_shape=jax.ShapeDtypeStruct((grid_rows, chans // 2), bf16),
        in_specs=[vmem] * 8 + [pl.BlockSpec(memory_space=pltpu.SMEM)],
        out_specs=vmem,
        scratch_shapes=[
            pltpu.VMEM((peers, grid_rows, chans), bf16),
            pltpu.VMEM((peers, 1, capacity), jnp.int32),
            pltpu.VMEM((peers, 1, capacity), jnp.int32),
            pltpu.VMEM((peers, 1, capacity), jnp.int32),
            pltpu.VMEM((2,) + w_src.shape, bf16),
            pltpu.VMEM((2, 1, hidden), f32),
            pltpu.VMEM((2, mesh_rows // 2, hidden), bf16),
            pltpu.VMEM((2,) + w_node.shape, bf16),
            pltpu.VMEM((2,) + w_dec.shape, bf16),
            pltpu.VMEM((peers, grid_rows // tile, mesh_rows // 2, tile), bf16),
            pltpu.VMEM((peers, grid_rows, mesh_rows), bf16),
            pltpu.VMEM((mesh_rows, capacity), HOT),
            pltpu.VMEM((2, mesh_rows // 2, hidden), f32),
            pltpu.VMEM((2, mesh_rows // 2, chans // 2), bf16),
            pltpu.VMEM((peers, mesh_rows, chans // 2), bf16),
            pltpu.VMEM((grid_rows, chans // 2), f32),
            dma((8,)), dma((5,)), dma((5,)), dma((2, peers)), dma((2, peers)),
            dma((2, CHUNKS)), dma((lines, CHUNKS)), dma((lines, CHUNKS)), dma((2, lines, CHUNKS)),
            dma((2, lines, CHUNKS)), dma((2, lines, CHUNKS)),
            dma((2, 2)), dma((lines, 2)), dma((lines, 2)), dma((2, lines, 2)), dma((1,)), dma((1,)), dma((peers,)), dma((peers,)),
        ],
        compiler_params=pltpu.CompilerParams(collective_id=0, has_side_effects=True),
    )(grid_state, w_src, bias_src[None, :], mesh_embed, w_node, w_dec, slot_src, slot_dst, slot_count)


def held_bytes(peers, grid_state, mesh_embed, *rest):
    grid_rows, chans = grid_state.shape
    mesh_rows = mesh_embed.shape[0]
    return 2 * peers * grid_rows * (chans + 2 * mesh_rows)


def per_device(grid_state, w_src, bias_src, mesh_embed, *rest):
    peers = lax.axis_size("graph")
    fits = (
        peers % 2 == 0
        and peers >= 4
        and lax.axis_size("chan") == 2
        and held_bytes(peers, grid_state, mesh_embed) <= VMEM_BUDGET
    )
    body = fused if fits else on_device
    return body(grid_state, w_src, bias_src, mesh_embed, *rest)


def solution(mesh):
    placed = (
        P(("member", "graph"), None),
        P(None, "chan"),
        P("chan"),
        P("graph", "chan"),
        P("chan", None),
        P("chan", None),
        P("graph", None, None),
        P(None, "graph", None),
        P(),
    )
    return jax.shard_map(
        per_device,
        mesh=mesh,
        in_specs=placed,
        out_specs=P(("member", "graph"), "chan"),
        check_vma=False,
    )
```

```python
import functools
import math

import jax
import jax.numpy as jnp
from jax import lax
from jax.experimental import pallas as pl
from jax.experimental.pallas import tpu as pltpu
from jax.sharding import PartitionSpec as P

CHUNKS = 4
HOT = jnp.float8_e4m3fn
VMEM_BUDGET = 48 * 2**20
MESH = pl.DeviceIdType.MESH
NT = (((1,), (1,)), ((), ()))


def edge_network(source_rows, w_src, bias_src):
    return jax.nn.silu(
        jnp.dot(source_rows, w_src, preferred_element_type=jnp.float32) + bias_src
    ).astype(jnp.bfloat16)


def segment_rows(values, indices, usable, row_count):
    slot_total = values.shape[0]
    width = values.shape[1]
    block_len = math.gcd(slot_total, 2048)
    block_count = slot_total // block_len
    targets = jnp.where(usable, indices, -1).reshape(block_count, block_len)
    pieces = values.reshape(block_count, block_len, width)
    row_ids = jnp.arange(row_count, dtype=jnp.int32)

    def add_block(summed, scan_item):
        row_target, piece_vals = scan_item
        one_hot = (row_ids[:, None] == row_target[None, :]).astype(jnp.bfloat16)
        return (summed + jnp.dot(one_hot, piece_vals, preferred_element_type=jnp.float32), None)

    result, unused = lax.scan(
        add_block, jnp.zeros((row_count, width), jnp.float32), (targets, pieces)
    )
    return result


def on_device(
    grid_state, w_src, bias_src, mesh_embed, w_node, w_dec, slot_src, slot_dst, slot_count
):
    peers = lax.axis_size("graph")
    own_index = lax.axis_index("graph")
    core_index = lax.axis_index("chan")
    capacity = slot_src.shape[2]
    positions = jnp.arange(capacity, dtype=jnp.int32)
    grid_rows = grid_state.shape[0]
    mesh_rows = mesh_embed.shape[0]
    sent_counts = lax.dynamic_slice_in_dim(slot_count, own_index, 1, 0)[0]
    recv_counts = lax.dynamic_slice_in_dim(slot_count, own_index, 1, 1)[:, 0]
    half_slots = capacity // 2
    chosen = lax.dynamic_slice_in_dim(slot_src[0], core_index * half_slots, half_slots, 1)
    picked = jnp.take(grid_state, chosen.reshape(-1), axis=0).reshape(
        peers, half_slots, grid_state.shape[1]
    )
    arrived = lax.all_to_all(picked, "graph", split_axis=0, concat_axis=0, tiled=True)
    joined = lax.all_gather(arrived, "chan", axis=1, tiled=True)
    messages = edge_network(joined.reshape(peers * capacity, grid_state.shape[1]), w_src, bias_src)
    arrive_ok = (positions[None, :] < recv_counts[:, None]).reshape(-1)
    dst_rows = slot_dst[:, 0, :].reshape(-1)
    aggregate = segment_rows(messages, dst_rows, arrive_ok, mesh_rows)
    partial_hidden = jnp.dot(
        aggregate.astype(jnp.bfloat16), w_node, preferred_element_type=jnp.float32
    )
    hidden_pre = lax.psum_scatter(partial_hidden, "chan", scatter_dimension=1, tiled=True)
    latent = (mesh_embed.astype(jnp.float32) + jax.nn.silu(hidden_pre)).astype(jnp.bfloat16)
    partial_proj = jnp.dot(latent, w_dec, preferred_element_type=jnp.float32)
    projected = lax.psum_scatter(partial_proj, "chan", scatter_dimension=1, tiled=True).astype(
        jnp.bfloat16
    )
    returned = jnp.take(projected, dst_rows, axis=0).reshape(peers, capacity, projected.shape[1])
    came_back = lax.all_to_all(returned, "graph", split_axis=0, concat_axis=0, tiled=True).reshape(
        peers * capacity, projected.shape[1]
    )
    send_ok = (positions[None, :] < sent_counts[:, None]).reshape(-1)
    decoded = segment_rows(came_back, slot_src[0].reshape(-1), send_ok, grid_rows)
    width_half = decoded.shape[1]
    own_cols = lax.dynamic_slice_in_dim(grid_state, core_index * width_half, width_half, 1)
    return (own_cols.astype(jnp.float32) + decoded).astype(jnp.bfloat16)


def silu(v):
    half = 0.5 * v
    return half + half * jnp.tanh(half)


def one_hot(first, rows, indices):
    row_ids = lax.broadcasted_iota(jnp.int32, (rows, indices.shape[1]), 0) + first
    return jnp.where(row_ids == indices, 1.0, 0.0).astype(HOT)


def graph_kernel(
    peers,
    x_ref, w_src_ref, bias_ref, embed_ref, w_node_ref, w_dec_ref, src_ref, dst_ref, count_ref,
    out_ref,
    x_all, src_own, src_in, dst_in, w_src_all, bias_all, embed_all, w_node_all, w_dec_all,
    enc, dec, hot, agg, proj, proj_all,
    local_sem, par_send, par_recv, idx_send, idx_recv,
    xo_send, xz_send, xy_send, x_recv, xm_send, xm_recv,
    po_send, pz_send, py_send, p_recv, pm_send, pm_recv, dec_send, dec_recv,
):
    lines = peers // 2
    me = lax.axis_index("graph")
    core = lax.axis_index("chan")
    mate = 1 - core
    line, side = me // 2, me % 2
    other = line * 2 + (1 - side)
    grid_rows, chans = x_ref.shape
    half_grid = grid_rows // 2
    piece = half_grid // CHUNKS
    mesh_rows = embed_ref.shape[0]
    half_mesh = mesh_rows // 2
    cols = chans // 2
    tile = enc.shape[3]
    tiles = grid_rows // tile
    capacity = src_ref.shape[2]

    def remote(src, dst, send, recv, graph, chan):
        return pltpu.make_async_remote_copy(
            src_ref=src, dst_ref=dst, send_sem=send, recv_sem=recv,
            device_id={"graph": graph, "chan": chan}, device_id_type=MESH,
        )

    barrier = pltpu.get_barrier_semaphore()
    for step in range(peers):
        for chan in range(2):
            if step == 0 and chan == 0:
                continue
            pl.semaphore_signal(
                barrier, inc=1,
                device_id={"graph": (me + step) % peers, "chan": (core + chan) % 2},
                device_id_type=MESH,
            )
    slots = lax.broadcasted_iota(jnp.int32, (1, capacity), 1)
    for to in range(peers):
        src_own[to] = jnp.where(slots < count_ref[me, to], src_ref[0, to : to + 1, :], -1)
    my_rows = pl.ds(pl.multiple_of(core * half_mesh, half_mesh), half_mesh)
    mate_rows = pl.ds(pl.multiple_of(mate * half_mesh, half_mesh), half_mesh)
    locals_ = [
        pltpu.make_async_copy(x_ref, x_all.at[me], local_sem.at[0]),
        pltpu.make_async_copy(w_src_ref, w_src_all.at[core], local_sem.at[1]),
        pltpu.make_async_copy(bias_ref, bias_all.at[core], local_sem.at[2]),
        pltpu.make_async_copy(embed_ref.at[my_rows], embed_all.at[core], local_sem.at[3]),
        pltpu.make_async_copy(w_node_ref, w_node_all.at[core], local_sem.at[4]),
        pltpu.make_async_copy(w_dec_ref, w_dec_all.at[core], local_sem.at[5]),
        pltpu.make_async_copy(src_own.at[me], src_in.at[me], local_sem.at[6]),
        pltpu.make_async_copy(dst_ref.at[me], dst_in.at[me], local_sem.at[7]),
    ]
    for copy in locals_:
        copy.start()
    for copy in locals_:
        copy.wait()
    pl.semaphore_wait(barrier, 2 * peers - 1)

    sends = []
    idx_copies = []
    for step in range(1, peers):
        to = (me + step) % peers
        for at, (ref, into) in enumerate(((src_own, src_in), (dst_ref, dst_in))):
            copy = remote(
                ref.at[to], into.at[me], idx_send.at[at, step], idx_recv.at[at, step], to, core
            )
            copy.start()
            idx_copies.append(copy)

    def nearest(at):
        return sorted((p for p in range(lines) if p != at), key=lambda p: (abs(p - at), p))

    from_line = [
        sum(jnp.where(line == at, nearest(at)[i], 0) for at in range(lines))
        for i in range(lines - 1)
    ]
    up, down = (line + 1) * 2 + side, (line - 1) * 2 + side

    def along(source, make):
        for going, target in (
            ((source <= line) & (line < lines - 1), up),
            ((source >= line) & (line > 0), down),
        ):
            @pl.when(going)
            def _(target=target):
                make(target).start()
            sends.append((going, functools.partial(make, target)))

    def begin(copy):
        copy.start()
        sends.append((None, lambda: copy))

    def x_part(shard, half, c):
        first = pl.multiple_of(half * half_grid, half_grid) + c * piece
        return x_all.at[shard, pl.ds(pl.multiple_of(first, piece), piece)]

    def x_own(c):
        first = pl.multiple_of(core * half_grid, half_grid) + c * piece
        return x_all.at[me, pl.ds(pl.multiple_of(first, piece), piece)]

    for c in range(CHUNKS):
        begin(remote(x_own(c), x_part(me, core, c), xy_send.at[line, c], x_recv.at[1, line, c], other, core))
        for at, (going, target) in enumerate(((line < lines - 1, up), (line > 0, down))):
            def make(c=c, at=at, target=target):
                return remote(
                    x_own(c), x_part(me, core, c), xo_send.at[at, c], x_recv.at[0, line, c],
                    target, core,
                )
            @pl.when(going)
            def _(make=make):
                make().start()
            sends.append((going, make))

    par_copies = [
        remote(w_src_all.at[core], w_src_all.at[core], par_send.at[0], par_recv.at[0], me, mate),
        remote(bias_all.at[core], bias_all.at[core], par_send.at[1], par_recv.at[1], me, mate),
        remote(embed_ref.at[mate_rows], embed_all.at[core], par_send.at[2], par_recv.at[2], me, mate),
        remote(w_node_all.at[core], w_node_all.at[core], par_send.at[3], par_recv.at[3], me, mate),
        remote(w_dec_all.at[core], w_dec_all.at[core], par_send.at[4], par_recv.at[4], me, mate),
    ]
    for copy in par_copies:
        copy.start()

    def to_mate(flip, source, c, shard):
        ref = x_part(shard, core, c)
        begin(remote(ref, ref, xm_send.at[flip, source, c], xm_recv.at[flip, source, c], me, mate))

    def relay(i, c):
        source = from_line[i]
        shard = source * 2 + side
        ref = x_part(shard, core, c)
        remote(ref, ref, xz_send.at[source, c], x_recv.at[0, source, c], me, mate).wait_recv()
        along(source, lambda target: remote(
            ref, ref, xz_send.at[source, c], x_recv.at[0, source, c], target, core))
        begin(remote(ref, ref, xy_send.at[source, c], x_recv.at[1, source, c], other, core))
        to_mate(0, source, c, shard)

    def take(source, c):
        shard = source * 2 + (1 - side)
        ref = x_part(shard, core, c)
        remote(ref, ref, xz_send.at[source, c], x_recv.at[1, source, c], me, mate).wait_recv()
        to_mate(1, source, c, shard)

    def build_enc(i, carry):
        shard = (me + i) % peers
        hot[: half_mesh, :] = one_hot(core * half_mesh, half_mesh, dst_ref[shard])
        for t in range(tiles):
            picks = one_hot(t * tile, tile, src_in[shard])
            enc[shard, t] = lax.dot_general(
                hot[: half_mesh, :], picks, NT, preferred_element_type=jnp.float32
            ).astype(jnp.bfloat16)
        return carry

    def build_dec(i, carry):
        shard = (me + i) % peers
        hot[...] = one_hot(0, mesh_rows, dst_in[shard])
        for t in range(half_grid // 256):
            first = pl.multiple_of(core * half_grid, half_grid) + t * 256
            picks = one_hot(first, 256, src_own[shard])
            dec[shard, pl.ds(pl.multiple_of(first, 256), 256), :] = lax.dot_general(
                picks, hot[...], NT, preferred_element_type=jnp.float32
            ).astype(jnp.bfloat16)
        return carry

    done = {build_enc: 0, build_dec: 0}
    pending = []

    def dec_copy(i, half):
        shard = (me + i) % peers
        ref = dec.at[shard, pl.ds(pl.multiple_of(half * half_grid, half_grid), half_grid)]
        return remote(ref, ref, dec_send.at[shard], dec_recv.at[shard], me, mate)

    def flush():
        while pending:
            begin(dec_copy(pending.pop(0), core))

    def build(which, count):
        first = done[which]
        last = min(first + count, peers)
        if last > first:
            flush()
            lax.fori_loop(first, last, which, 0)
            if which is build_dec:
                pending.extend(range(first, last))
        done[which] = last

    def encode(shard):
        def step(t, carry):
            rows = pl.ds(pl.multiple_of(t * tile, tile), tile)
            for h in range(2):
                pre = jnp.dot(
                    x_all[shard, rows, :], w_src_all[h], preferred_element_type=jnp.float32
                ) + bias_all[h]
                agg[h] += jnp.dot(
                    enc[shard, t], silu(pre).astype(jnp.bfloat16),
                    preferred_element_type=jnp.float32,
                )
            return carry
        lax.fori_loop(0, tiles, step, 0)

    def encode_from(flip, source):
        shard = source * 2 + (side if flip == 0 else 1 - side)
        for c in range(CHUNKS):
            ref = x_part(shard, mate, c)
            remote(ref, ref, xm_send.at[flip, source, c], xm_recv.at[flip, source, c], me, mate).wait_recv()
        encode(shard)

    agg[...] = jnp.zeros_like(agg)
    out_ref[...] = x_all[me, :, pl.ds(pl.multiple_of(core * cols, cols), cols)].astype(jnp.float32)
    build(build_enc, 1)
    build(build_dec, 1)
    for copy in par_copies:
        copy.wait()
    encode(me)
    for copy in idx_copies:
        copy.wait()
    flush()
    build(build_enc, peers // 4)
    last = lines - 2
    for i in range(lines - 1):
        for c in range(CHUNKS):
            relay(i, c)
            if i == 0:
                build(build_enc, peers // CHUNKS // 4)
            else:
                take(from_line[i - 1], c)
                if c < CHUNKS - 1:
                    build(build_dec, 1)
        if i == 0:
            for c in range(CHUNKS):
                take(line, c)
            build(build_enc, peers)
        elif i == 1:
            encode_from(0, from_line[0])
            encode_from(1, line)
            build(build_dec, 1)
        else:
            encode_from(0, from_line[i - 1])
            encode_from(1, from_line[i - 2])
            build(build_dec, 1)
    encode_from(0, from_line[last])
    take(from_line[last], 0)
    encode_from(1, from_line[last - 1])
    for c in range(1, CHUNKS):
        take(from_line[last], c)
    encode_from(1, from_line[last])

    hidden = sum(
        jnp.dot(agg[h].astype(jnp.bfloat16), w_node_all[h], preferred_element_type=jnp.float32)
        for h in range(2)
    )
    width = hidden.shape[1] // 2
    projected = sum(
        jnp.dot(
            (
                embed_all[h].astype(jnp.float32) + silu(hidden[:, h * width : (h + 1) * width])
            ).astype(jnp.bfloat16),
            w_dec_all[h], preferred_element_type=jnp.float32,
        )
        for h in range(2)
    ).astype(jnp.bfloat16)
    for h in range(2):
        proj[h] = projected[:, h * cols : (h + 1) * cols]

    own_copy = pltpu.make_async_copy(proj.at[core], proj_all.at[me, my_rows], local_sem.at[0])
    own_copy.start()
    into = proj_all.at[me, my_rows]
    for flip in range(2):
        chan = (core + flip) % 2
        begin(remote(proj.at[chan], into, py_send.at[line, flip], p_recv.at[1, line, core], other, chan))
        for at, (going, target) in enumerate(((line < lines - 1, up), (line > 0, down))):
            def make(flip=flip, chan=chan, at=at, target=target):
                return remote(
                    proj.at[chan], into, po_send.at[at, flip], p_recv.at[0, line, core],
                    target, chan,
                )
            @pl.when(going)
            def _(make=make):
                make().start()
            sends.append((going, make))
    begin(remote(proj.at[mate], into, pm_send.at[0], pm_recv.at[0], me, mate))

    def p_part(shard, half):
        return proj_all.at[shard, pl.ds(pl.multiple_of(half * half_mesh, half_mesh), half_mesh)]

    def p_wait(flip, source, half):
        ref = p_part(source * 2 + (side if flip == 0 else 1 - side), half)
        remote(ref, ref, pz_send.at[source, half], p_recv.at[flip, source, half], me, mate).wait_recv()

    def p_relay(i):
        source = from_line[i]
        for half in (core, mate):
            p_wait(0, source, half)
            ref = p_part(source * 2 + side, half)
            along(source, lambda target, half=half, ref=ref: remote(
                ref, ref, pz_send.at[source, half], p_recv.at[0, source, half], target, core))
            begin(remote(ref, ref, py_send.at[source, half], p_recv.at[1, source, half], other, core))

    def decode(shard):
        def step(t, carry):
            rows = pl.ds(pl.multiple_of(t * half_grid, half_grid), half_grid)
            out_ref[rows, :] += jnp.dot(
                dec[shard, rows, :], proj_all[shard], preferred_element_type=jnp.float32
            )
            return carry
        lax.fori_loop(0, 2, step, 0)

    flush()
    left = peers - done[build_dec]
    for i in range(lines - 1):
        build(build_dec, -(-left // (lines - 1)))
        p_relay(i)
    flush()
    for i in range(peers):
        dec_copy(i, mate).wait_recv()
    own_copy.wait()
    remote(proj.at[mate], into, pm_send.at[0], pm_recv.at[0], me, mate).wait_recv()
    decode(me)
    for i in range(lines - 1):
        decode(from_line[i] * 2 + side)
    for source in [line] + from_line:
        for half in (core, mate):
            p_wait(1, source, half)
        decode(source * 2 + 1 - side)

    for going, make in sends:
        if going is None:
            make().wait_send()
        else:
            @pl.when(going)
            def _(make=make):
                make().wait_send()


def fused(grid_state, w_src, bias_src, mesh_embed, w_node, w_dec, slot_src, slot_dst, slot_count):
    peers = lax.axis_size("graph")
    capacity = slot_src.shape[2]
    grid_rows, chans = grid_state.shape
    mesh_rows = mesh_embed.shape[0]
    hidden = w_src.shape[1]
    lines = peers // 2
    bf16, f32 = jnp.bfloat16, jnp.float32
    dma = pltpu.SemaphoreType.DMA
    vmem = pl.BlockSpec(memory_space=pltpu.VMEM)
    tile = grid_rows // 2
    return pl.pallas_call(
        functools.partial(graph_kernel, peers),
        out_shape=jax.ShapeDtypeStruct((grid_rows, chans // 2), f32),
        in_specs=[pl.BlockSpec(memory_space=pl.ANY)] * 6 + [vmem] * 2 + [pl.BlockSpec(memory_space=pltpu.SMEM)],
        out_specs=vmem,
        scratch_shapes=[
            pltpu.VMEM((peers, grid_rows, chans), bf16),
            pltpu.VMEM((peers, 1, capacity), jnp.int32),
            pltpu.VMEM((peers, 1, capacity), jnp.int32),
            pltpu.VMEM((peers, 1, capacity), jnp.int32),
            pltpu.VMEM((2,) + w_src.shape, bf16),
            pltpu.VMEM((2, 1, hidden), f32),
            pltpu.VMEM((2, mesh_rows // 2, hidden), bf16),
            pltpu.VMEM((2,) + w_node.shape, bf16),
            pltpu.VMEM((2,) + w_dec.shape, bf16),
            pltpu.VMEM((peers, grid_rows // tile, mesh_rows // 2, tile), bf16),
            pltpu.VMEM((peers, grid_rows, mesh_rows), bf16),
            pltpu.VMEM((mesh_rows, capacity), HOT),
            pltpu.VMEM((2, mesh_rows // 2, hidden), f32),
            pltpu.VMEM((2, mesh_rows // 2, chans // 2), bf16),
            pltpu.VMEM((peers, mesh_rows, chans // 2), bf16),
            dma((8,)), dma((5,)), dma((5,)), dma((2, peers)), dma((2, peers)),
            dma((2, CHUNKS)), dma((lines, CHUNKS)), dma((lines, CHUNKS)), dma((2, lines, CHUNKS)),
            dma((2, lines, CHUNKS)), dma((2, lines, CHUNKS)),
            dma((2, 2)), dma((lines, 2)), dma((lines, 2)), dma((2, lines, 2)), dma((1,)), dma((1,)), dma((peers,)), dma((peers,)),
        ],
        compiler_params=pltpu.CompilerParams(collective_id=0, has_side_effects=True),
    )(grid_state, w_src, bias_src[None, :], mesh_embed, w_node, w_dec, slot_src, slot_dst, slot_count).astype(bf16)


def held_bytes(peers, grid_state, mesh_embed, *rest):
    grid_rows, chans = grid_state.shape
    mesh_rows = mesh_embed.shape[0]
    return 2 * peers * grid_rows * (chans + 2 * mesh_rows)


def per_device(grid_state, w_src, bias_src, mesh_embed, *rest):
    peers = lax.axis_size("graph")
    fits = (
        peers % 2 == 0
        and peers >= 4
        and lax.axis_size("chan") == 2
        and held_bytes(peers, grid_state, mesh_embed) <= VMEM_BUDGET
    )
    body = fused if fits else on_device
    return body(grid_state, w_src, bias_src, mesh_embed, *rest)


def solution(mesh):
    placed = (
        P(("member", "graph"), None),
        P(None, "chan"),
        P("chan"),
        P("graph", "chan"),
        P("chan", None),
        P("chan", None),
        P("graph", None, None),
        P(None, "graph", None),
        P(),
    )
    return jax.shard_map(
        per_device,
        mesh=mesh,
        in_specs=placed,
        out_specs=P(("member", "graph"), "chan"),
        check_vma=False,
    )
```
